32 devices in a mesh: tm: 8 (over z, y), obs: 4 (over x, core).
Axes of the slice: x: 2, y: 2, z: 4, core: 2. Of those that a mesh axis runs over, the one named last changes fastest.
Arguments:
- trajectory: bfloat16 [8, 64, 256, 128], P('tm', 'obs'), may hold values from -6 to 6
- weights: bfloat16 [1024, 128, 256], P(('tm', 'obs')), may hold values from -0.375 to 0.375
- observed: bfloat16 [1024, 128, 128], P(('tm', 'obs')), may hold values from -9 to 9
- window: int32 [1024, 1], P(('tm', 'obs')), may hold values from 0 to 7; in each aligned block of 32 rows (0 to 31, 32 to 63, ...) at most 4 rows name the same one
- block: int32 [1024], P(('tm', 'obs')), may hold values from 0 to 15
- counts: int32 [1024], P(('tm', 'obs')), may hold values from 32 to 128, as said below
- flags: int32 [1024, 128], P(('tm', 'obs')), may hold values 0 or 1
- inv_error: float32 [128], replicated, may hold values from 0.5 to 2
Outputs:
- departures: bfloat16 [1024, 128, 128], P(('tm', 'obs'))
- window_bias: float32 [8, 128], P('tm')
- window_chi: float32 [8, 128], P('tm')
The draws below stay inside these ranges and needn't reach their ends.
Inputs may be any that keep to these rules, and one draw needn't show every extreme that they name: Among the 32 groups of one device, no sub-window is named by more than 4. `counts`: among the 32 groups of one device, one has all 128 slots live.
All inputs are finite; a program needn't handle non-finite values. No bound on the sum of `flags` on one device may be relied on, other than what follows from the above.
Results may differ from the reference program's by a relative error of at most 0.001.
Values may be sent and summed in bfloat16 or wider, within the bound.
A program may use at most 64 MiB of HBM per device.

```python
import math
import jax
import jax.numpy as jnp
import numpy as np
from jax import lax

LEV = 128
G = 256
BL = 16
CAPB = 128
NGRP = 32
GCAP = 4
NT = 8
NB = 64
NGRP_ALL = 1024
N_TM = 8
N_OBS = 4


def draw_counts(key, part):
    devices = N_TM * N_OBS
    first_key = jax.random.fold_in(key, 11)
    second_key = jax.random.fold_in(key, 23)
    values = jax.random.randint(first_key, (devices, NGRP), CAPB // 4, CAPB + 1)
    full_at = jax.random.randint(second_key, (devices,), 0, NGRP)
    column = jnp.arange(NGRP, dtype=jnp.int32)[None, :]
    values = jnp.where(column == full_at[:, None], CAPB, values)
    return values.reshape(devices * NGRP).astype(jnp.int32)


def place_ends(array, rng, least, high):
    place = [jax.random.randint(jax.random.fold_in(rng, axis), (), 0, length) for axis, length in enumerate(array.shape)]
    widest = array.shape.index(max(array.shape))
    neighbour = place[:widest] + [(place[widest] + 1) % array.shape[widest]] + place[widest + 1:]
    return array.at[tuple(place)].set(least).at[tuple(neighbour)].set(high)


def block_scale(own_key, shape, pieces, low, largest):
    loudness, own = 1.0, jax.random.fold_in(own_key, 6)
    for position, shards_of in pieces:
        steps = jnp.exp(jax.random.uniform(jax.random.fold_in(own, position), (shards_of,), jnp.float32, low / len(pieces), largest / len(pieces)))
        loudness = loudness * jnp.repeat(steps, shape[position] // shards_of).reshape([-1 if axis == position else 1 for axis in range(len(shape))])
    return loudness


def shared_out(stream_key, own, number, rows, number_of, top, bound, lean):
    ranking = jax.random.permutation(stream_key, number_of)
    packed, usual = load_shares(number_of, rows * top, bound, lean, True), load_shares(number_of, rows * top, bound, lean, False)
    places = jnp.arange(number_of)

    def named(sizes, turn):
        used = int((sizes > 0).sum())
        fixed = max(1, used // 4)
        shifted = fixed + (places - fixed + turn * (used - fixed)) % max(1, number_of - fixed)
        return jnp.zeros((number_of,), jnp.int32).at[ranking[jnp.where(places < fixed, places, shifted)]].set(jnp.asarray(sizes, jnp.int32))

    sizes = jnp.where(number % 4 == 0, named(packed, number // 4), named(usual, number - number // 4 - 1))
    mixed = jax.random.permutation(jax.random.fold_in(own, 3), number_of)
    source_of, sink = mixed[0:number_of // 2 * 2:2], mixed[1:number_of // 2 * 2:2]
    margin = jnp.minimum(sizes[source_of] - 1, bound - sizes[sink]) // 2
    margin = jnp.where((source_of == ranking[0]) | (sink == ranking[0]) | (sizes[sink] == 0), 0, jnp.maximum(margin, 0))
    shifted = jax.random.randint(jax.random.fold_in(own, 4), (number_of // 2,), 0, 1 << 20) % (margin + 1)
    sizes = sizes.at[source_of].add(-shifted).at[sink].add(shifted)
    items = jnp.searchsorted(jnp.cumsum(sizes), jnp.arange(rows * top), side="right").astype(jnp.int32)
    table = items.reshape(top, rows).T
    table = table[jax.random.permutation(jax.random.fold_in(own, 1), rows)]
    turn = jax.random.randint(jax.random.fold_in(own, 2), (rows, 1), 0, top)
    return jnp.take_along_axis(table, (jnp.arange(top)[None, :] + turn) % top, axis=1)


def load_shares(count, total, bound, lean, full):
    loads = [(1 << 20) // math.isqrt(rank ** lean) + 1 for rank in range(1, count + 1)]
    largest = bound if full else min(bound, max(-(-total // count), total * loads[0] // sum(loads)))
    least = 1 if total - largest >= count - 1 else 0
    given, surplus = [largest] + [least] * (count - 1), total - largest - least * (count - 1)
    while surplus > 0:
        candidates = [i for i in range(1, count) if given[i] < largest] or [i for i in range(1, count) if given[i] < bound]
        mass, remaining = sum([loads[i] for i in candidates]), surplus
        for i in candidates:
            extra = min(bound - given[i], max(1, remaining * loads[i] // mass), surplus)
            given[i] = given[i] + extra
            surplus = surplus - extra
    return np.array(given)


def bell_draw(rng, shape, deviation, most, shards=(), kind=jnp.bfloat16):
    entries = jax.random.normal(rng, shape, jnp.float32) * deviation
    if len(shards) > 0:
        entries = block_scale(rng, shape, shards, -0.22, 0.18) * entries
    return jnp.clip(entries, min=-most, max=most).astype(kind)


def setup_inputs(seed: int = 0) -> dict:
    keys = jax.random.split(jax.random.key(seed), 9)
    trajectory = bell_draw(keys[0], (NT, NB, G, LEV), 1.0, 6.0, ((0, 8), (1, 4)))
    weights = bell_draw(keys[1], (NGRP_ALL, CAPB, G), G ** -0.5, 0.375, ((0, 32),))
    observed = bell_draw(keys[2], (NGRP_ALL, CAPB, LEV), 1.5, 9.0, ((0, 32),))
    window_keys = jax.random.split(jax.random.fold_in(keys[3], 1), NGRP_ALL // NGRP)
    window_turns = jax.random.permutation(jax.random.fold_in(keys[3], 3), NGRP_ALL // NGRP)
    window = jax.vmap(lambda own, number: shared_out(jax.random.fold_in(keys[3], 2), own, number, NGRP, NT, 1, GCAP, 2))(window_keys, window_turns).reshape((NGRP_ALL, 1))
    block = place_ends(jax.random.randint(keys[4], (NGRP_ALL,), 0, BL), jax.random.fold_in(keys[4], 1), 0, BL - 1).astype(jnp.int32)
    counts = draw_counts(jax.random.fold_in(keys[8], 71), 0)
    flags = place_ends((jax.random.randint(keys[6], (NGRP_ALL, CAPB), 0, 4) < 3).astype(jnp.int32), jax.random.fold_in(keys[6], 1), 0, 1)
    inv_error = jnp.clip(jnp.exp(jax.random.uniform(keys[7], (LEV,), jnp.float32, math.log(0.5), math.log(2.0))), 0.5, 2.0)
    return {"trajectory": trajectory, "weights": weights, "observed": observed, "window": window, "block": block, "counts": counts, "flags": flags, "inv_error": inv_error}


def reference(trajectory, weights, observed, window, block, counts, flags, inv_error):
    devices = N_TM * N_OBS
    nwin = N_TM
    w_dev = weights.reshape(devices, NGRP, CAPB, G)
    y_dev = observed.reshape(devices, NGRP, CAPB, LEV)
    win_dev = window.reshape(devices, NGRP).astype(jnp.int32)
    blk_dev = block.reshape(devices, NGRP).astype(jnp.int32)
    cnt_dev = counts.reshape(devices, NGRP).astype(jnp.int32)
    flg_dev = flags.reshape(devices, NGRP, CAPB).astype(jnp.int32)
    dev_ids = jnp.arange(devices, dtype=jnp.int32)

    def one_device(items):
        dev, w_here, y_here, win_here, blk_here, cnt_here, flg_here = items
        region = (dev % N_OBS).astype(jnp.int32)
        slab = lax.dynamic_slice_in_dim(trajectory, region * BL, BL, 1)
        picked = slab[win_here, blk_here].astype(jnp.float32)
        hx = jnp.einsum('gop,gpl->gol', w_here.astype(jnp.float32), picked)
        slot_ids = jnp.arange(CAPB, dtype=jnp.int32)
        used = jnp.where(slot_ids[None, :] < cnt_here[:, None], flg_here, 0).astype(jnp.float32)
        departure = used[:, :, None] * (y_here.astype(jnp.float32) - hx) * inv_error[None, None, :]
        member = (win_here[:, None] == jnp.arange(nwin, dtype=jnp.int32)[None, :]).astype(jnp.float32)
        sum_one = jnp.einsum('gt,gl->tl', member, lax.optimization_barrier(jnp.sum(departure, 1)), precision=lax.Precision.HIGHEST)
        sum_two = jnp.einsum('gt,gl->tl', member, lax.optimization_barrier(jnp.sum(departure * departure, 1)), precision=lax.Precision.HIGHEST)
        kept = jnp.einsum('gt,g->t', member, lax.optimization_barrier(jnp.sum(used, 1)), precision=lax.Precision.HIGHEST)
        return (departure.astype(jnp.bfloat16), sum_one, sum_two, kept)
    deps, ones, twos, kepts = lax.map(one_device, (dev_ids, w_dev, y_dev, win_dev, blk_dev, cnt_dev, flg_dev))
    sum_one = lax.optimization_barrier(jnp.sum(ones, 0))
    sum_two = lax.optimization_barrier(jnp.sum(twos, 0))
    kept = lax.optimization_barrier(jnp.sum(kepts, 0))
    departures = deps.reshape(NGRP * devices, CAPB, LEV)
    window_bias = sum_one / jnp.sqrt(kept[:, None] + 1.0)
    window_chi = sum_two / (kept[:, None] + 1.0)
    return (departures, window_bias, window_chi)
```

```python
import functools

import jax
import jax.numpy as jnp
from jax import lax
from jax.experimental import pallas as pl
from jax.experimental.pallas import tpu as pltpu
from jax.sharding import PartitionSpec as P

GCAP = 4
MESH = pl.DeviceIdType.MESH


def flip(index, pattern):
    bit = 1
    moved = index
    while bit <= pattern:
        if pattern & bit:
            moved = moved + bit * (1 - 2 * ((index // bit) % 2))
        bit *= 2
    return moved


def phases(windows):
    half, quarter = windows // 2, max(1, windows // 4)
    far = list(range(half, windows))
    return far[:1] + list(range(quarter, half)) + far[1:] + list(range(1, quarter))


def last_hits(win_of, value_of, groups, wanted, start):
    def step(g, held):
        hit = win_of(g) == wanted
        shifted = (value_of(g),) + held[:-1]
        return tuple(jnp.where(hit, new, old) for new, old in zip(shifted, held))

    return lax.fori_loop(0, groups, step, (jnp.int32(start),) * GCAP, unroll=8)


def kernel(
    windows, regions, groups, slots, levels,
    traj, weights, observed, win_in, blk_in, counts_in, flags_in, inv_in,
    dep_out, total_out,
    slab, wts, obs, send, recv, mask, dep_slot, dep_v, stat_send, stat_recv,
    idx, own, table, slot_tab, counts, flags, inv,
    in_sems, out_sem, idx_send, idx_recv, dat_send, dat_recv, st_send, st_recv,
):
    me = lax.axis_index("tm")
    my_region = lax.axis_index("obs")
    everyone = windows * regions
    flat = me * regions + my_region
    order = phases(windows)

    small = [
        pltpu.make_async_copy(src, dst, in_sems.at[3 + n])
        for n, (src, dst) in enumerate(
            ((win_in, own.at[0]), (blk_in, own.at[1]), (counts_in, counts), (flags_in, flags), (inv_in, inv))
        )
    ]
    for copy in small:
        copy.start()
    slab_in = pltpu.make_async_copy(traj.at[0], slab, in_sems.at[0])
    slab_in.start()
    wts_in = pltpu.make_async_copy(weights, wts, in_sems.at[1])
    obs_in = pltpu.make_async_copy(observed, obs, in_sems.at[2])

    barrier = pltpu.get_barrier_semaphore()

    partners = [(flip(me, d), my_region) for d in order]
    partners += [(me, (my_region + r) % regions) for r in range(1, regions)]
    for partner in partners:
        pl.semaphore_signal(barrier, inc=1, device_id=partner, device_id_type=MESH)
    small[0].wait()
    small[1].wait()
    pl.semaphore_wait(barrier, len(partners))

    requests = []
    for j, d in enumerate(order):
        target = (flip(me, d), my_region)
        copy = pltpu.make_async_remote_copy(
            src_ref=own, dst_ref=idx.at[j],
            send_sem=idx_send.at[j], recv_sem=idx_recv.at[j],
            device_id=target, device_id_type=MESH,
        )
        copy.start()
        requests.append(copy)
    wts_in.start()
    obs_in.start()

    slab_in.wait()
    moves = []
    for j, d in enumerate(order):
        requests[j].wait_recv()
        named = last_hits(
            lambda g, j=j: idx[j, 0, g], lambda g, j=j: idx[j, 1, g], groups, me, 0
        )
        for k in range(GCAP):
            send[j * GCAP + k] = slab[named[k]]
        copy = pltpu.make_async_remote_copy(
            src_ref=send.at[pl.ds(j * GCAP, GCAP)],
            dst_ref=recv.at[pl.ds(j * GCAP, GCAP)],
            send_sem=dat_send.at[j], recv_sem=dat_recv.at[j],
            device_id=(flip(me, d), my_region), device_id_type=MESH,
        )
        copy.start()
        moves.append(copy)

    for copy in small[2:]:
        copy.wait()

    def fill(w, carry):
        named = last_hits(lambda g: own[0, g], lambda g: g, groups, w, -1)
        for k in range(GCAP):
            table[w * GCAP + k] = named[k]
        return carry

    lax.fori_loop(0, windows, fill, 0)

    def place(g, carry):
        base = own[0, g] * GCAP
        rank = jnp.int32(0)
        for k in range(1, GCAP):
            rank = rank + jnp.where(table[base + k] == g, k, 0)
        slot_tab[g] = base + rank
        return carry

    lax.fori_loop(0, groups, place, 0)

    down = lax.broadcasted_iota(jnp.int32, (slots, slots), 0)
    across = lax.broadcasted_iota(jnp.int32, (slots, slots), 1)
    lane = lax.broadcasted_iota(jnp.int32, (1, slots), 1)
    ones = jnp.ones((slots, levels), jnp.bfloat16)

    def spread(g, carry):
        row = jnp.where(lane < counts[g], flags[pl.ds(g, 1), :], 0)
        diagonal = jnp.where(down == across, jnp.broadcast_to(row, (slots, slots)), 0)
        mask[g] = jnp.dot(
            diagonal.astype(jnp.float32).astype(jnp.bfloat16), ones,
            preferred_element_type=jnp.float32,
        )
        return carry

    lax.fori_loop(0, groups, spread, 0)
    wts_in.wait()
    obs_in.wait()
    inverse = inv[...]
    padded = windows * GCAP > groups

    def check(w, blocks):
        one = jnp.zeros((1, levels), jnp.float32)
        two = jnp.zeros((1, levels), jnp.float32)
        kept = jnp.zeros((1, levels), jnp.float32)
        for k in range(GCAP):
            named = table[w * GCAP + k]
            g = jnp.maximum(named, 0)
            hx = jnp.dot(wts[g], blocks(k, g), preferred_element_type=jnp.float32)
            keep = mask[g]
            if padded:
                keep = keep * jnp.where(named >= 0, 1.0, 0.0)
            dep = keep * (obs[g].astype(jnp.float32) - hx) * inverse
            dep_slot[w * GCAP + k] = dep.astype(jnp.bfloat16)
            one = one + jnp.sum(dep, 0, keepdims=True)
            two = two + jnp.sum(dep * dep, 0, keepdims=True)
            kept = kept + jnp.sum(keep, 0, keepdims=True)
        stat_send[w] = jnp.concatenate(
            [one, two, kept, jnp.zeros((5, levels), jnp.float32)], 0
        )

    def share(w, first):
        for r in range(first, regions):
            copy = pltpu.make_async_remote_copy(
                src_ref=stat_send.at[w], dst_ref=stat_recv.at[flat],
                send_sem=st_send, recv_sem=st_recv,
                device_id=(w, (my_region + r) % regions), device_id_type=MESH,
            )
            copy.start()

    check(me, lambda k, g: slab[own[1, g]])
    share(me, 1)
    for j, d in sorted(enumerate(order), key=lambda item: item[1] >= windows // 2):
        w = flip(me, d)
        moves[j].wait_recv()
        check(w, lambda k, g, j=j: recv[j * GCAP + k])
        share(w, 0)

    def permute(g, carry):
        dep_v[g] = dep_slot[slot_tab[g]]
        return carry

    lax.fori_loop(0, groups, permute, 0, unroll=4)
    dep_out[...] = dep_v[...]


    for j in range(len(order)):
        requests[j].wait_send()
        moves[j].wait_send()

    rest = pl.ds(0, everyone - 1)
    arrived = pltpu.make_async_remote_copy(
        src_ref=stat_recv.at[rest], dst_ref=stat_recv.at[rest],
        send_sem=st_send, recv_sem=st_recv,
        device_id=(flip(me, 1), my_region), device_id_type=MESH,
    )
    arrived.wait_recv()
    stat_recv[flat] = stat_send[me]
    total_out[...] = jnp.sum(stat_recv[...], 0)
    arrived.wait_send()


def per_device(trajectory, weights, observed, window, block, counts, flags, inv_error):
    windows = lax.axis_size("tm")
    regions = lax.axis_size("obs")
    groups, slots, columns = weights.shape
    levels = observed.shape[2]
    blocks = trajectory.shape[1]
    peers = windows - 1
    dma = pltpu.SemaphoreType.DMA
    hbm = pl.BlockSpec(memory_space=pl.ANY)
    vmem = pl.BlockSpec(memory_space=pltpu.VMEM)
    b16, f32, i32 = jnp.bfloat16, jnp.float32, jnp.int32
    departures, total = pl.pallas_call(
        functools.partial(kernel, windows, regions, groups, slots, levels),
        out_shape=(
            pltpu.VMEM((groups, slots, levels), b16),
            pltpu.VMEM((8, levels), f32),
        ),
        in_specs=[hbm] * 8,
        out_specs=(vmem, vmem),
        scratch_shapes=[
            pltpu.VMEM((blocks, columns, levels), b16),
            pltpu.VMEM((groups, slots, columns), b16),
            pltpu.VMEM((groups, slots, levels), b16),
            pltpu.VMEM((peers * GCAP, columns, levels), b16),
            pltpu.VMEM((peers * GCAP, columns, levels), b16),
            pltpu.VMEM((groups, slots, levels), f32),
            pltpu.VMEM((windows * GCAP, slots, levels), b16),
            pltpu.VMEM((groups, slots, levels), b16),
            pltpu.VMEM((windows, 8, levels), f32),
            pltpu.VMEM((windows * regions, 8, levels), f32),
            pltpu.SMEM((peers, 2, groups), i32),
            pltpu.SMEM((2, groups), i32),
            pltpu.SMEM((windows * GCAP,), i32),
            pltpu.SMEM((groups,), i32),
            pltpu.SMEM((groups,), i32),
            pltpu.VMEM((groups, slots), i32),
            pltpu.VMEM((1, levels), f32),
            dma((8,)),
            dma,
            dma((peers,)),
            dma((peers,)),
            dma((peers,)),
            dma((peers,)),
            dma,
            dma,
        ],
        compiler_params=pltpu.CompilerParams(
            collective_id=0, has_side_effects=True, vmem_limit_bytes=60 * 1024 * 1024
        ),
    )(
        trajectory, weights, observed, window[:, 0], block, counts, flags,
        inv_error.reshape(1, levels),
    )
    weight = total[2:3] + 1.0
    return (departures, total[0:1] / jnp.sqrt(weight), total[1:2] / weight)


def solution(mesh):
    return jax.shard_map(
        per_device,
        mesh=mesh,
        in_specs=(
            P("tm", "obs", None, None),
            P(("tm", "obs"), None, None),
            P(("tm", "obs"), None, None),
            P(("tm", "obs"), None),
            P(("tm", "obs")),
            P(("tm", "obs")),
            P(("tm", "obs"), None),
            P(),
        ),
        out_specs=(P(("tm", "obs"), None, None), P("tm", None), P("tm", None)),
        check_vma=False,
    )
```

```python
import functools

import jax
import jax.numpy as jnp
from jax import lax
from jax.experimental import pallas as pl
from jax.experimental.pallas import tpu as pltpu
from jax.sharding import PartitionSpec as P

GCAP = 4
MESH = pl.DeviceIdType.MESH

ASK = ((1, 2, 3, 4, 5, 6, 7), (2, 3, 1, 6), (4, 5, 6, 7, 1, 2, 3), (2, 3, 4, 5, 6, 7, 1))
AHEAD_AFTER = (None, 6, 7, None)
OUTER_GIVE, OUTER_TAKE = (1, 4, 5, 6, 7, 2, 3), (1, 2, 3, 6, 7, 4, 5)
INNER_GIVE, INNER_LATE, INNER_TAKE = (2, 1, 3), (4, 5, 7, 6), ((1, 4, 5), (2, 3, 7, 6))
ACROSS, AHEAD = 6, 4


def flip(index, pattern):
    bit, moved = 1, index
    while bit <= 64:
        moved = moved + bit * ((pattern // bit) % 2) * (1 - 2 * ((index // bit) % 2))
        bit *= 2
    return moved


def last_hits(win_of, value_of, groups, wanted, start):
    def step(g, held):
        hit = win_of(g) == wanted
        shifted = (value_of(g),) + held[:-1]
        return tuple(jnp.where(hit, new, old) for new, old in zip(shifted, held))

    return lax.fori_loop(0, groups, step, (jnp.int32(start),) * GCAP, unroll=8)


def kernel(
    windows, regions, groups, slots, levels,
    traj, weights, observed, win_in, blk_in, counts_in, flags_in, inv_in,
    dep_out, total_out,
    slab, wts, obs, send, recv, head, pre, on_out, on_in, mask, dep_slot, stat_send, stat_recv,
    idx, own, table, slot_tab, counts, flags, inv,
    in_sems, ready_tm, ready_obs, idx_send, idx_recv, pass_send, dat_send, dat_recv,
    pre_send, pre_recv, on_send, on_recv, st_send, st_recv,
):
    me = lax.axis_index("tm")
    my_region = lax.axis_index("obs")
    everyone = windows * regions
    flat = me * regions + my_region
    tuned = windows == 8
    inner = ((me // 2 + 1) // 2) % 2 == 1
    blocks, columns = slab.shape[0], slab.shape[1]
    ahead = columns // AHEAD if tuned else 0

    small = [
        pltpu.make_async_copy(src, dst, in_sems.at[3 + n])
        for n, (src, dst) in enumerate(
            ((win_in, own.at[0]), (blk_in, own.at[1]), (counts_in, counts), (flags_in, flags), (inv_in, inv))
        )
    ]
    slab_in = pltpu.make_async_copy(traj.at[0], slab, in_sems.at[0])
    head_in = pltpu.make_async_copy(traj.at[0, :, pl.ds(0, columns // AHEAD)], head, in_sems.at[8])
    wts_in = pltpu.make_async_copy(weights, wts, in_sems.at[1])
    obs_in = pltpu.make_async_copy(observed, obs, in_sems.at[2])

    barrier = pltpu.get_barrier_semaphore()
    tm_peers = [(d, flip(me, d)) for d in range(1, windows)]
    obs_peers = [(r, flip(my_region, r)) for r in range(2, regions)]
    pl.semaphore_signal(barrier, inc=1, device_id=(me, flip(my_region, 1)), device_id_type=MESH)
    for d, peer in tm_peers:
        @pl.when(peer > me)
        def _():
            pl.semaphore_signal(barrier, inc=1, device_id=(peer, my_region), device_id_type=MESH)
    for r, peer in obs_peers:
        @pl.when(peer > my_region)
        def _():
            pl.semaphore_signal(barrier, inc=1, device_id=(me, peer), device_id_type=MESH)
    small[0].start()
    small[1].start()
    if tuned:
        head_in.start()
    slab_in.start()
    for copy in small[2:]:
        copy.start()
    pl.semaphore_wait(barrier, 1 + me + 2 * (my_region // 2))
    for d, peer in tm_peers:
        hears = peer < me
        if tuned and d in (4, 5, 7):
            hears = jnp.logical_and(hears, peer // 2 != 1)

        @pl.when(hears)
        def _():
            pl.semaphore_signal(ready_tm.at[d - 1], inc=1, device_id=(peer, my_region), device_id_type=MESH)
    for r, peer in obs_peers:
        @pl.when(peer < my_region)
        def _():
            pl.semaphore_signal(ready_obs, inc=1, device_id=(me, peer), device_id_type=MESH)
    small[0].wait()
    small[1].wait()

    def request(d):
        return pltpu.make_async_remote_copy(
            src_ref=own, dst_ref=idx.at[d],
            send_sem=idx_send, recv_sem=idx_recv.at[d - 1],
            device_id=(flip(me, d), my_region), device_id_type=MESH,
        )

    def ask(d):
        @pl.when(flip(me, d) > me)
        def _():
            pl.semaphore_wait(ready_tm.at[d - 1], 1)

        request(d).start()

    def pass_on(e):
        return pltpu.make_async_remote_copy(
            src_ref=idx.at[ACROSS], dst_ref=idx.at[e ^ ACROSS],
            send_sem=pass_send, recv_sem=idx_recv.at[(e ^ ACROSS) - 1],
            device_id=(flip(me, e), my_region), device_id_type=MESH,
        )

    def move(d, k, count=1, first=0):
        part, rows = pl.ds(d * GCAP + k, count), pl.ds(first, columns - first)
        return pltpu.make_async_remote_copy(
            src_ref=send.at[part, rows], dst_ref=recv.at[part, rows],
            send_sem=dat_send, recv_sem=dat_recv.at[d - 1 if d != ACROSS or k == 0 else windows - 2 + k],
            device_id=(flip(me, d), my_region), device_id_type=MESH,
        )

    def moved(count):
        part = send.at[pl.ds(0, count)]
        pltpu.make_async_remote_copy(
            src_ref=part, dst_ref=part, send_sem=dat_send, recv_sem=dat_recv.at[0],
            device_id=(flip(me, 1), my_region), device_id_type=MESH,
        ).wait_send()

    def give(d, first=0, skip_heard=None):
        if d != skip_heard:
            request(d).wait_recv()
        named = last_hits(lambda g: idx[d, 0, g], lambda g: idx[d, 1, g], groups, me, 0)
        for k in range(GCAP):
            send[d * GCAP + k, first:] = slab[named[k], first:]
            move(d, k, 1, first).start()

    def run_ahead():
        return pltpu.make_async_remote_copy(
            src_ref=head, dst_ref=pre, send_sem=pre_send, recv_sem=pre_recv,
            device_id=(flip(me, ACROSS), my_region), device_id_type=MESH,
        )

    def hand_on(e):
        return pltpu.make_async_remote_copy(
            src_ref=on_out.at[e], dst_ref=on_in.at[e ^ ACROSS],
            send_sem=on_send, recv_sem=on_recv.at[e % 2],
            device_id=(flip(me, e), my_region), device_id_type=MESH,
        )

    def relay():
        run_ahead().wait_recv()
        for e in (1, 2, 3):
            named = last_hits(
                lambda g: idx[e, 0, g], lambda g: idx[e, 1, g], groups, flip(me, ACROSS), 0
            )
            for k in range(GCAP):
                on_out[e, k] = pre[named[k]]
            hand_on(e).start()

    if tuned:
        for z, order in enumerate(ASK):
            @pl.when(me // 2 == z)
            def _():
                for d in order:
                    ask(d)
                    if d == AHEAD_AFTER[z]:
                        head_in.wait()
                        run_ahead().start()
                if z in (0, 3):
                    head_in.wait()
                if z == 2:
                    request(ACROSS).wait_recv()
                    for e in (1, 2, 3):
                        pass_on(e).start()
    else:
        for d in range(1, windows):
            ask(d)
    later = regions - 2 - 2 * (my_region // 2)

    @pl.when(later > 0)
    def _():
        pl.semaphore_wait(ready_obs, later)

    slab_in.wait()
    wts_in.start()
    obs_in.start()
    if tuned:
        @pl.when(inner)
        def _():
            for d in INNER_GIVE:
                give(d)

        @pl.when(jnp.logical_not(inner))
        def _():
            for d in OUTER_GIVE:
                give(d)
    else:
        for d in range(1, windows):
            give(d)

    for copy in small[2:]:
        copy.wait()

    def fill(w, carry):
        named = last_hits(lambda g: own[0, g], lambda g: g, groups, w, -1)
        for k in range(GCAP):
            table[w * GCAP + k] = named[k]
        return carry

    lax.fori_loop(0, windows, fill, 0)

    def place(g, carry):
        base = own[0, g] * GCAP
        rank = jnp.int32(0)
        for k in range(1, GCAP):
            rank = rank + jnp.where(table[base + k] == g, k, 0)
        slot_tab[g] = base + rank
        return carry

    lax.fori_loop(0, groups, place, 0)

    down = lax.broadcasted_iota(jnp.int32, (slots, slots), 0)
    across = lax.broadcasted_iota(jnp.int32, (slots, slots), 1)
    lane = lax.broadcasted_iota(jnp.int32, (1, slots), 1)
    ones = jnp.ones((slots, levels), jnp.bfloat16)

    def spread(g, carry):
        row = jnp.where(lane < counts[g], flags[pl.ds(g, 1), :], 0)
        diagonal = jnp.where(down == across, jnp.broadcast_to(row, (slots, slots)), 0)
        mask[g] = jnp.dot(
            diagonal.astype(jnp.float32).astype(jnp.bfloat16), ones,
            preferred_element_type=jnp.float32,
        )
        return carry

    lax.fori_loop(0, groups, spread, 0)
    wts_in.wait()
    obs_in.wait()
    inverse = inv[...]
    padded = windows * GCAP > groups

    def check(w, blocks):
        one = jnp.zeros((1, levels), jnp.float32)
        two = jnp.zeros((1, levels), jnp.float32)
        kept = jnp.zeros((1, levels), jnp.float32)
        for k in range(GCAP):
            named = table[w * GCAP + k]
            g = jnp.maximum(named, 0)
            hx = jnp.dot(wts[g], blocks(k, g), preferred_element_type=jnp.float32)
            keep = mask[g]
            if padded:
                keep = keep * jnp.where(named >= 0, 1.0, 0.0)
            dep = keep * (obs[g].astype(jnp.float32) - hx) * inverse
            dep_slot[w * GCAP + k] = dep.astype(jnp.bfloat16)
            one = one + jnp.sum(dep, 0, keepdims=True)
            two = two + jnp.sum(dep * dep, 0, keepdims=True)
            kept = kept + jnp.sum(keep, 0, keepdims=True)
        stat_send[w] = jnp.concatenate(
            [one, two, kept, jnp.zeros((5, levels), jnp.float32)], 0
        )

    def share(w, first):
        for r in range(first, regions):
            copy = pltpu.make_async_remote_copy(
                src_ref=stat_send.at[w], dst_ref=stat_recv.at[flat],
                send_sem=st_send, recv_sem=st_recv,
                device_id=(w, flip(my_region, r)), device_id_type=MESH,
            )
            copy.start()

    check(me, lambda k, g: slab[own[1, g]])
    share(me, 1)

    def take(d, first=0):
        w = flip(me, d)
        if first and d != ACROSS:
            hand_on(d ^ ACROSS).wait_recv()

        if d != ACROSS:
            move(d, 0, GCAP, first).wait_recv()

        def arrived(k, g):
            if first:
                recv[d * GCAP + k, :first] = pre[own[1, g]] if d == ACROSS else on_in[d, k]
            if d == ACROSS:
                move(d, k, 1, first).wait_recv()
            return recv[d * GCAP + k]

        check(w, arrived)
        share(w, 0)

    if tuned:
        @pl.when(inner)
        def _():
            for d in INNER_TAKE[0]:
                take(d)
            for d in INNER_LATE:
                if d == ACROSS:
                    @pl.when(me // 2 == 1)
                    def _():
                        request(ACROSS).wait_recv()
                give(d, ahead, ACROSS)

            relay()
            for d in INNER_TAKE[1]:
                take(d, ahead if d in (6, 7) else 0)
            moved(len(INNER_GIVE) * GCAP + len(INNER_LATE) * GCAP * (columns - ahead) // columns)
            run_ahead().wait_send()
            part = on_out.at[pl.ds(1, 3)]
            pltpu.make_async_remote_copy(
                src_ref=part, dst_ref=part, send_sem=on_send, recv_sem=on_recv.at[0],
                device_id=(flip(me, 1), my_region), device_id_type=MESH,
            ).wait_send()

        @pl.when(jnp.logical_not(inner))
        def _():
            for d in OUTER_TAKE:
                take(d, ahead if d in (4, 5) else 0)
            moved(len(OUTER_GIVE) * GCAP)
    else:
        for d in range(1, windows):
            take(d)
        moved((windows - 1) * GCAP)

    def permute(g, carry):
        dep_out[g] = dep_slot[slot_tab[g]]
        return carry

    lax.fori_loop(0, groups, permute, 0, unroll=4)

    def asked(count, sem):
        part = idx.at[pl.ds(0, count)]
        pltpu.make_async_remote_copy(
            src_ref=part, dst_ref=part, send_sem=sem, recv_sem=idx_recv.at[0],
            device_id=(flip(me, 1), my_region), device_id_type=MESH,
        ).wait_send()

    if tuned:
        for z, order in enumerate(ASK):
            @pl.when(me // 2 == z)
            def _():
                asked(len(order), idx_send)
                if z == 2:
                    asked(3, pass_send)
    else:
        asked(windows - 1, idx_send)

    rest = pl.ds(0, everyone - 1)
    everything = pltpu.make_async_remote_copy(
        src_ref=stat_recv.at[rest], dst_ref=stat_recv.at[rest],
        send_sem=st_send, recv_sem=st_recv,
        device_id=(flip(me, 1), my_region), device_id_type=MESH,
    )
    everything.wait_recv()
    stat_recv[flat] = stat_send[me]
    total_out[...] = jnp.sum(stat_recv[...], 0)
    everything.wait_send()


def per_device(trajectory, weights, observed, window, block, counts, flags, inv_error):
    windows = lax.axis_size("tm")
    regions = lax.axis_size("obs")
    groups, slots, columns = weights.shape
    levels = observed.shape[2]
    blocks = trajectory.shape[1]
    dma = pltpu.SemaphoreType.DMA
    regular = pltpu.SemaphoreType.REGULAR
    hbm = pl.BlockSpec(memory_space=pl.ANY)
    vmem = pl.BlockSpec(memory_space=pltpu.VMEM)
    b16, f32, i32 = jnp.bfloat16, jnp.float32, jnp.int32
    departures, total = pl.pallas_call(
        functools.partial(kernel, windows, regions, groups, slots, levels),
        out_shape=(
            pltpu.VMEM((groups, slots, levels), b16),
            pltpu.VMEM((8, levels), f32),
        ),
        in_specs=[hbm] * 8,
        out_specs=(vmem, vmem),
        scratch_shapes=[
            pltpu.VMEM((blocks, columns, levels), b16),
            pltpu.VMEM((groups, slots, columns), b16),
            pltpu.VMEM((groups, slots, levels), b16),
            pltpu.VMEM((windows * GCAP, columns, levels), b16),
            pltpu.VMEM((windows * GCAP, columns, levels), b16),
            pltpu.VMEM((blocks, columns // AHEAD, levels), b16),
            pltpu.VMEM((blocks, columns // AHEAD, levels), b16),
            pltpu.VMEM((windows, GCAP, columns // AHEAD, levels), b16),
            pltpu.VMEM((windows, GCAP, columns // AHEAD, levels), b16),
            pltpu.VMEM((groups, slots, levels), f32),
            pltpu.VMEM((windows * GCAP, slots, levels), b16),
            pltpu.VMEM((windows, 8, levels), f32),
            pltpu.VMEM((windows * regions, 8, levels), f32),
            pltpu.SMEM((windows, 2, groups), i32),
            pltpu.SMEM((2, groups), i32),
            pltpu.SMEM((windows * GCAP,), i32),
            pltpu.SMEM((groups,), i32),
            pltpu.SMEM((groups,), i32),
            pltpu.VMEM((groups, slots), i32),
            pltpu.VMEM((1, levels), f32),
            dma((9,)),
            regular((windows - 1,)),
            regular,
            dma,
            dma((windows - 1,)),
            dma,
            dma,
            dma((windows + GCAP - 2,)),
            dma,
            dma,
            dma,
            dma((2,)),
            dma,
            dma,
        ],
        compiler_params=pltpu.CompilerParams(
            collective_id=0, has_side_effects=True, vmem_limit_bytes=60 * 1024 * 1024
        ),
    )(
        trajectory, weights, observed, window[:, 0], block, counts, flags,
        inv_error.reshape(1, levels),
    )
    weight = total[2:3] + 1.0
    return (departures, total[0:1] / jnp.sqrt(weight), total[1:2] / weight)


def solution(mesh):
    return jax.shard_map(
        per_device,
        mesh=mesh,
        in_specs=(
            P("tm", "obs", None, None),
            P(("tm", "obs"), None, None),
            P(("tm", "obs"), None, None),
            P(("tm", "obs"), None),
            P(("tm", "obs")),
            P(("tm", "obs")),
            P(("tm", "obs"), None),
            P(),
        ),
        out_specs=(P(("tm", "obs"), None, None), P("tm", None), P("tm", None)),
        check_vma=False,
    )
```

```python
import functools

import jax
import jax.numpy as jnp
from jax import lax
from jax.experimental import pallas as pl
from jax.experimental.pallas import tpu as pltpu
from jax.sharding import PartitionSpec as P

GCAP = 4
MESH = pl.DeviceIdType.MESH

ASK = ((1, 2, 3, 4, 5, 6, 7), (6, 2, 3, 1), (4, 5, 7, 6, 1, 2, 3), (2, 3, 4, 5, 6, 7, 1))
AHEAD_AFTER = (None, 6, 6, None)
OUTER_GIVE, OUTER_TAKE = (1, 4, 5, 6, 7, 2, 3), (1, 2, 3, 6, 7, 4, 5)
INNER_GIVE, INNER_LATE, INNER_TAKE = (2, 1, 3), (4, 5, 7, 6), ((1, 4, 5), (2, 3, 7, 6))
ACROSS, AHEAD = 6, 4


def flip(index, pattern):
    bit, moved = 1, index
    while bit <= 64:
        moved = moved + bit * ((pattern // bit) % 2) * (1 - 2 * ((index // bit) % 2))
        bit *= 2
    return moved


def last_hits(win_of, value_of, groups, wanted, start):
    def step(g, held):
        hit = win_of(g) == wanted
        shifted = (value_of(g),) + held[:-1]
        return tuple(jnp.where(hit, new, old) for new, old in zip(shifted, held))

    return lax.fori_loop(0, groups, step, (jnp.int32(start),) * GCAP, unroll=8)


def kernel(
    windows, regions, groups, slots, levels,
    traj, weights, observed, win_in, blk_in, counts_in, flags_in, inv_in,
    dep_out, total_out,
    slab, wts, obs, send, recv, head, pre, on_out, on_in, mask, dep_slot, stat_send, stat_recv,
    idx, own, table, slot_tab, counts, flags, inv,
    in_sems, ready_tm, ready_obs, idx_send, idx_recv, pass_send, dat_send, dat_recv,
    pre_send, pre_recv, on_send, on_recv, st_send, st_recv,
):
    me = lax.axis_index("tm")
    my_region = lax.axis_index("obs")
    everyone = windows * regions
    flat = me * regions + my_region
    tuned = windows == 8
    inner_flag = ((me // 2 + 1) // 2) % 2
    inner = inner_flag == 1
    blocks, columns = slab.shape[0], slab.shape[1]
    ahead = columns // AHEAD if tuned else 0

    small = [
        pltpu.make_async_copy(src, dst, in_sems.at[3 + n])
        for n, (src, dst) in enumerate(
            ((win_in, own.at[0]), (blk_in, own.at[1]), (counts_in, counts), (flags_in, flags), (inv_in, inv))
        )
    ]
    slab_in = pltpu.make_async_copy(traj.at[0], slab, in_sems.at[0])
    head_in = pltpu.make_async_copy(traj.at[0, :, pl.ds(0, columns // AHEAD)], head, in_sems.at[8])
    wts_in = pltpu.make_async_copy(weights, wts, in_sems.at[1])
    obs_in = pltpu.make_async_copy(observed, obs, in_sems.at[2])

    barrier = pltpu.get_barrier_semaphore()

    def greets(d):
        before = flip(me, d) > me
        if tuned and d == ACROSS:
            return jnp.logical_xor(before, inner)
        return before

    tm_peers = [(d, flip(me, d)) for d in range(1, windows)]
    obs_peers = [(r, flip(my_region, r)) for r in range(2, regions)]
    pl.semaphore_signal(barrier, inc=1, device_id=(me, flip(my_region, 1)), device_id_type=MESH)
    for d, peer in tm_peers:
        @pl.when(greets(d))
        def _():
            pl.semaphore_signal(barrier, inc=1, device_id=(peer, my_region), device_id_type=MESH)
    for r, peer in obs_peers:
        @pl.when(peer > my_region)
        def _():
            pl.semaphore_signal(barrier, inc=1, device_id=(me, peer), device_id_type=MESH)
    small[0].start()
    small[1].start()
    if tuned:
        head_in.start()
    slab_in.start()
    for copy in small[2:]:
        copy.start()
    early = 1 + me + 2 * (my_region // 2)
    if tuned:
        early = early + inner_flag * (3 - 2 * (me // 2))
    pl.semaphore_wait(barrier, early)
    for d, peer in tm_peers:
        hears = jnp.logical_not(greets(d))
        if tuned and d in (4, 5, 7):
            hears = jnp.logical_and(hears, peer // 2 != 1)

        @pl.when(hears)
        def _():
            pl.semaphore_signal(ready_tm.at[d - 1], inc=1, device_id=(peer, my_region), device_id_type=MESH)
    for r, peer in obs_peers:
        @pl.when(peer < my_region)
        def _():
            pl.semaphore_signal(ready_obs, inc=1, device_id=(me, peer), device_id_type=MESH)
    small[0].wait()
    small[1].wait()

    def request(d):
        return pltpu.make_async_remote_copy(
            src_ref=own, dst_ref=idx.at[d],
            send_sem=idx_send, recv_sem=idx_recv.at[d - 1],
            device_id=(flip(me, d), my_region), device_id_type=MESH,
        )

    def ask(d):
        @pl.when(greets(d))
        def _():
            pl.semaphore_wait(ready_tm.at[d - 1], 1)

        request(d).start()

    def pass_on(e):
        return pltpu.make_async_remote_copy(
            src_ref=idx.at[ACROSS], dst_ref=idx.at[e ^ ACROSS],
            send_sem=pass_send, recv_sem=idx_recv.at[(e ^ ACROSS) - 1],
            device_id=(flip(me, e), my_region), device_id_type=MESH,
        )

    def move(d, k, count=1, first=0):
        part, rows = pl.ds(d * GCAP + k, count), pl.ds(first, columns - first)
        return pltpu.make_async_remote_copy(
            src_ref=send.at[part, rows], dst_ref=recv.at[part, rows],
            send_sem=dat_send, recv_sem=dat_recv.at[d - 1 if d != ACROSS or k == 0 else windows - 2 + k],
            device_id=(flip(me, d), my_region), device_id_type=MESH,
        )

    def moved(count):
        part = send.at[pl.ds(0, count)]
        pltpu.make_async_remote_copy(
            src_ref=part, dst_ref=part, send_sem=dat_send, recv_sem=dat_recv.at[0],
            device_id=(flip(me, 1), my_region), device_id_type=MESH,
        ).wait_send()

    def give(d, first=0, skip_heard=None):
        if d != skip_heard:
            request(d).wait_recv()
        named = last_hits(lambda g: idx[d, 0, g], lambda g: idx[d, 1, g], groups, me, 0)
        for k in range(GCAP):
            send[d * GCAP + k, first:] = slab[named[k], first:]
            if d == ACROSS:
                move(d, k, 1, first).start()
        if d != ACROSS:
            move(d, 0, GCAP, first).start()

    def run_ahead():
        return pltpu.make_async_remote_copy(
            src_ref=head, dst_ref=pre, send_sem=pre_send, recv_sem=pre_recv,
            device_id=(flip(me, ACROSS), my_region), device_id_type=MESH,
        )

    def hand_on(e):
        return pltpu.make_async_remote_copy(
            src_ref=on_out.at[e], dst_ref=on_in.at[e ^ ACROSS],
            send_sem=on_send, recv_sem=on_recv.at[e % 2],
            device_id=(flip(me, e), my_region), device_id_type=MESH,
        )

    def relay():
        run_ahead().wait_recv()
        for e in (1, 2, 3):
            named = last_hits(
                lambda g: idx[e, 0, g], lambda g: idx[e, 1, g], groups, flip(me, ACROSS), 0
            )
            for k in range(GCAP):
                on_out[e, k] = pre[named[k]]
            hand_on(e).start()

    if tuned:
        for z, order in enumerate(ASK):
            @pl.when(me // 2 == z)
            def _():
                for d in order:
                    ask(d)
                    if d == AHEAD_AFTER[z]:
                        head_in.wait()
                        run_ahead().start()
                if z in (0, 3):
                    head_in.wait()
                if z == 2:
                    request(ACROSS).wait_recv()
                    for e in (1, 2, 3):
                        pass_on(e).start()
    else:
        for d in range(1, windows):
            ask(d)
    later = regions - 2 - 2 * (my_region // 2)

    @pl.when(later > 0)
    def _():
        pl.semaphore_wait(ready_obs, later)

    slab_in.wait()
    wts_in.start()
    obs_in.start()
    if tuned:
        @pl.when(inner)
        def _():
            for d in INNER_GIVE:
                give(d)

        @pl.when(jnp.logical_not(inner))
        def _():
            for d in OUTER_GIVE:
                give(d)
    else:
        for d in range(1, windows):
            give(d)

    for copy in small[2:]:
        copy.wait()

    def fill(w, carry):
        named = last_hits(lambda g: own[0, g], lambda g: g, groups, w, -1)
        for k in range(GCAP):
            table[w * GCAP + k] = named[k]
        return carry

    lax.fori_loop(0, windows, fill, 0)

    def place(g, carry):
        base = own[0, g] * GCAP
        rank = jnp.int32(0)
        for k in range(1, GCAP):
            rank = rank + jnp.where(table[base + k] == g, k, 0)
        slot_tab[g] = base + rank
        return carry

    lax.fori_loop(0, groups, place, 0)

    down = lax.broadcasted_iota(jnp.int32, (slots, slots), 0)
    across = lax.broadcasted_iota(jnp.int32, (slots, slots), 1)
    lane = lax.broadcasted_iota(jnp.int32, (1, slots), 1)
    ones = jnp.ones((slots, levels), jnp.bfloat16)

    def spread(g, carry):
        row = jnp.where(lane < counts[g], flags[pl.ds(g, 1), :], 0)
        diagonal = jnp.where(down == across, jnp.broadcast_to(row, (slots, slots)), 0)
        mask[g] = jnp.dot(
            diagonal.astype(jnp.float32).astype(jnp.bfloat16), ones,
            preferred_element_type=jnp.float32,
        )
        return carry

    lax.fori_loop(0, groups, spread, 0)
    wts_in.wait()
    obs_in.wait()
    inverse = inv[...]
    padded = windows * GCAP > groups

    def check(w, blocks):
        one = jnp.zeros((1, levels), jnp.float32)
        two = jnp.zeros((1, levels), jnp.float32)
        kept = jnp.zeros((1, levels), jnp.float32)
        for k in range(GCAP):
            named = table[w * GCAP + k]
            g = jnp.maximum(named, 0)
            hx = jnp.dot(wts[g], blocks(k, g), preferred_element_type=jnp.float32)
            keep = mask[g]
            if padded:
                keep = keep * jnp.where(named >= 0, 1.0, 0.0)
            dep = keep * (obs[g].astype(jnp.float32) - hx) * inverse
            dep_slot[w * GCAP + k] = dep.astype(jnp.bfloat16)
            one = one + jnp.sum(dep, 0, keepdims=True)
            two = two + jnp.sum(dep * dep, 0, keepdims=True)
            kept = kept + jnp.sum(keep, 0, keepdims=True)
        stat_send[w] = jnp.concatenate(
            [one, two, kept, jnp.zeros((5, levels), jnp.float32)], 0
        )

    def share(w, first):
        for r in reversed(range(first, regions)):
            copy = pltpu.make_async_remote_copy(
                src_ref=stat_send.at[w], dst_ref=stat_recv.at[flat],
                send_sem=st_send, recv_sem=st_recv,
                device_id=(w, flip(my_region, r)), device_id_type=MESH,
            )
            copy.start()

    check(me, lambda k, g: slab[own[1, g]])
    share(me, 1)

    def take(d, first=0):
        w = flip(me, d)
        if first and d != ACROSS:
            hand_on(d ^ ACROSS).wait_recv()

        if d != ACROSS:
            move(d, 0, GCAP, first).wait_recv()

        def arrived(k, g):
            if first:
                recv[d * GCAP + k, :first] = pre[own[1, g]] if d == ACROSS else on_in[d, k]
            if d == ACROSS:
                move(d, k, 1, first).wait_recv()
            return recv[d * GCAP + k]

        check(w, arrived)
        share(w, 0)

    if tuned:
        @pl.when(inner)
        def _():
            for d in INNER_TAKE[0]:
                take(d)
            for d in INNER_LATE:
                if d == ACROSS:
                    @pl.when(me // 2 == 1)
                    def _():
                        request(ACROSS).wait_recv()
                give(d, ahead, ACROSS)

            relay()
            for d in INNER_TAKE[1]:
                take(d, ahead if d in (6, 7) else 0)
            moved(len(INNER_GIVE) * GCAP + len(INNER_LATE) * GCAP * (columns - ahead) // columns)
            run_ahead().wait_send()
            part = on_out.at[pl.ds(1, 3)]
            pltpu.make_async_remote_copy(
                src_ref=part, dst_ref=part, send_sem=on_send, recv_sem=on_recv.at[0],
                device_id=(flip(me, 1), my_region), device_id_type=MESH,
            ).wait_send()

        @pl.when(jnp.logical_not(inner))
        def _():
            for d in OUTER_TAKE:
                take(d, ahead if d in (4, 5) else 0)
            moved(len(OUTER_GIVE) * GCAP)
    else:
        for d in range(1, windows):
            take(d)
        moved((windows - 1) * GCAP)

    def permute(g, carry):
        dep_out[g] = dep_slot[slot_tab[g]]
        return carry

    lax.fori_loop(0, groups, permute, 0, unroll=4)

    def asked(count, sem):
        part = idx.at[pl.ds(0, count)]
        pltpu.make_async_remote_copy(
            src_ref=part, dst_ref=part, send_sem=sem, recv_sem=idx_recv.at[0],
            device_id=(flip(me, 1), my_region), device_id_type=MESH,
        ).wait_send()

    if tuned:
        for z, order in enumerate(ASK):
            @pl.when(me // 2 == z)
            def _():
                asked(len(order), idx_send)
                if z == 2:
                    asked(3, pass_send)
    else:
        asked(windows - 1, idx_send)

    rest = pl.ds(0, everyone - 1)
    everything = pltpu.make_async_remote_copy(
        src_ref=stat_recv.at[rest], dst_ref=stat_recv.at[rest],
        send_sem=st_send, recv_sem=st_recv,
        device_id=(flip(me, 1), my_region), device_id_type=MESH,
    )
    everything.wait_recv()
    stat_recv[flat] = stat_send[me]
    total_out[...] = jnp.sum(stat_recv[...], 0)
    everything.wait_send()


def finish(dep, total, dep_out, bias_out, chi_out, ratio, sems):
    whole = pltpu.make_async_copy(dep, dep_out, sems.at[0])
    whole.start()
    weight = total[2:3] + 1.0
    ratio[0:1] = total[0:1] / jnp.sqrt(weight)
    ratio[8:9] = total[1:2] / weight
    bias = pltpu.make_async_copy(ratio.at[0:1], bias_out, sems.at[1])
    chi = pltpu.make_async_copy(ratio.at[8:9], chi_out, sems.at[2])
    bias.start()
    chi.start()
    bias.wait()
    chi.wait()
    whole.wait()


def per_device(trajectory, weights, observed, window, block, counts, flags, inv_error):
    windows = lax.axis_size("tm")
    regions = lax.axis_size("obs")
    groups, slots, columns = weights.shape
    levels = observed.shape[2]
    blocks = trajectory.shape[1]
    dma = pltpu.SemaphoreType.DMA
    regular = pltpu.SemaphoreType.REGULAR
    hbm = pl.BlockSpec(memory_space=pl.ANY)
    vmem = pl.BlockSpec(memory_space=pltpu.VMEM)
    b16, f32, i32 = jnp.bfloat16, jnp.float32, jnp.int32
    departures, total = pl.pallas_call(
        functools.partial(kernel, windows, regions, groups, slots, levels),
        out_shape=(
            pltpu.VMEM((groups, slots, levels), b16),
            pltpu.VMEM((8, levels), f32),
        ),
        in_specs=[hbm] * 8,
        out_specs=(vmem, vmem),
        scratch_shapes=[
            pltpu.VMEM((blocks, columns, levels), b16),
            pltpu.VMEM((groups, slots, columns), b16),
            pltpu.VMEM((groups, slots, levels), b16),
            pltpu.VMEM((windows * GCAP, columns, levels), b16),
            pltpu.VMEM((windows * GCAP, columns, levels), b16),
            pltpu.VMEM((blocks, columns // AHEAD, levels), b16),
            pltpu.VMEM((blocks, columns // AHEAD, levels), b16),
            pltpu.VMEM((windows, GCAP, columns // AHEAD, levels), b16),
            pltpu.VMEM((windows, GCAP, columns // AHEAD, levels), b16),
            pltpu.VMEM((groups, slots, levels), f32),
            pltpu.VMEM((windows * GCAP, slots, levels), b16),
            pltpu.VMEM((windows, 8, levels), f32),
            pltpu.VMEM((windows * regions, 8, levels), f32),
            pltpu.SMEM((windows, 2, groups), i32),
            pltpu.SMEM((2, groups), i32),
            pltpu.SMEM((windows * GCAP,), i32),
            pltpu.SMEM((groups,), i32),
            pltpu.SMEM((groups,), i32),
            pltpu.VMEM((groups, slots), i32),
            pltpu.VMEM((1, levels), f32),
            dma((9,)),
            regular((windows - 1,)),
            regular,
            dma,
            dma((windows - 1,)),
            dma,
            dma,
            dma((windows + GCAP - 2,)),
            dma,
            dma,
            dma,
            dma((2,)),
            dma,
            dma,
        ],
        compiler_params=pltpu.CompilerParams(
            collective_id=0, has_side_effects=True, vmem_limit_bytes=60 * 1024 * 1024
        ),
    )(
        trajectory, weights, observed, window[:, 0], block, counts, flags,
        inv_error.reshape(1, levels),
    )
    return pl.pallas_call(
        finish,
        out_shape=(
            jax.ShapeDtypeStruct((groups, slots, levels), b16),
            jax.ShapeDtypeStruct((1, levels), f32),
            jax.ShapeDtypeStruct((1, levels), f32),
        ),
        in_specs=[vmem, vmem],
        out_specs=(hbm, hbm, hbm),
        scratch_shapes=[pltpu.VMEM((16, levels), f32), dma((3,))],
    )(*(pltpu.with_memory_space_constraint(x, pltpu.VMEM) for x in (departures, total)))


def solution(mesh):
    return jax.shard_map(
        per_device,
        mesh=mesh,
        in_specs=(
            P("tm", "obs", None, None),
            P(("tm", "obs"), None, None),
            P(("tm", "obs"), None, None),
            P(("tm", "obs"), None),
            P(("tm", "obs")),
            P(("tm", "obs")),
            P(("tm", "obs"), None),
            P(),
        ),
        out_specs=(P(("tm", "obs"), None, None), P("tm", None), P("tm", None)),
        check_vma=False,
    )
```

```python
import functools

import jax
import jax.numpy as jnp
from jax import lax
from jax.experimental import pallas as pl
from jax.experimental.pallas import tpu as pltpu
from jax.sharding import PartitionSpec as P

GCAP = 4
MESH = pl.DeviceIdType.MESH

ASK = ((1, 2, 3, 4, 5, 6, 7), (6, 2, 3, 1), (4, 5, 7, 6, 1, 2, 3), (2, 3, 4, 5, 6, 7, 1))
AHEAD_AFTER = (None, 6, 6, None)
OUTER_GIVE, OUTER_TAKE = (1, 5, 4, 7, 6, 3, 2), (1, 2, 3, 7, 6, 4, 5)
INNER_GIVE, INNER_LATE, INNER_TAKE = (2, 3, 1), (4, 5, 7, 6), ((1, 5, 4), (3, 2, 7, 6))
ACROSS, AHEAD = 6, 4


def flip(index, pattern):
    bit, moved = 1, index
    while bit <= 64:
        moved = moved + bit * ((pattern // bit) % 2) * (1 - 2 * ((index // bit) % 2))
        bit *= 2
    return moved


def last_hits(win_of, value_of, groups, wanted, start):
    def step(g, held):
        hit = win_of(g) == wanted
        shifted = (value_of(g),) + held[:-1]
        return tuple(jnp.where(hit, new, old) for new, old in zip(shifted, held))

    return lax.fori_loop(0, groups, step, (jnp.int32(start),) * GCAP, unroll=8)


def kernel(
    windows, regions, groups, slots, levels,
    traj, weights, observed, win_in, blk_in, counts_in, flags_in, inv_in,
    dep_out, total_out,
    slab, wts, obs, send, recv, head, pre, on_out, on_in, mask, dep_slot, stat_send, stat_recv,
    idx, own, table, slot_tab, counts, flags, inv,
    in_sems, ready_tm, ready_obs, idx_send, idx_recv, pass_send, dat_send, dat_recv,
    pre_send, pre_recv, on_send, on_recv, st_send, st_recv,
):
    me = lax.axis_index("tm")
    my_region = lax.axis_index("obs")
    everyone = windows * regions
    flat = me * regions + my_region
    tuned = windows == 8
    inner_flag = ((me // 2 + 1) // 2) % 2
    inner = inner_flag == 1
    blocks, columns = slab.shape[0], slab.shape[1]
    ahead = columns // AHEAD if tuned else 0

    small = [
        pltpu.make_async_copy(src, dst, in_sems.at[3 + n])
        for n, (src, dst) in enumerate(
            ((win_in, own.at[0]), (blk_in, own.at[1]), (counts_in, counts), (flags_in, flags), (inv_in, inv))
        )
    ]
    slab_in = pltpu.make_async_copy(traj.at[0], slab, in_sems.at[0])
    head_in = pltpu.make_async_copy(traj.at[0, :, pl.ds(0, columns // AHEAD)], head, in_sems.at[8])
    wts_in = pltpu.make_async_copy(weights, wts, in_sems.at[1])
    obs_in = pltpu.make_async_copy(observed, obs, in_sems.at[2])

    barrier = pltpu.get_barrier_semaphore()

    def opposite(d):
        return jnp.logical_and(inner, tuned and d == ACROSS)

    tm_peers = [(d, flip(me, d)) for d in range(1, windows)]
    obs_peers = [(r, flip(my_region, r)) for r in range(2, regions)]
    pl.semaphore_signal(barrier, inc=1, device_id=(me, flip(my_region, 1)), device_id_type=MESH)
    for d, peer in tm_peers:
        @pl.when(jnp.logical_or(peer > me, opposite(d)))
        def _():
            pl.semaphore_signal(barrier, inc=1, device_id=(peer, my_region), device_id_type=MESH)
    for r, peer in obs_peers:
        @pl.when(peer > my_region)
        def _():
            pl.semaphore_signal(barrier, inc=1, device_id=(me, peer), device_id_type=MESH)
    small[0].start()
    small[1].start()
    if tuned:
        head_in.start()
    slab_in.start()
    for copy in small[2:]:
        copy.start()
    early = 1 + me + 2 * (my_region // 2)
    if tuned:
        early = early + inner_flag * (2 - me // 2)
    pl.semaphore_wait(barrier, early)
    for d, peer in tm_peers:
        hears = jnp.logical_and(peer < me, jnp.logical_not(opposite(d)))
        if tuned and d in (4, 5, 7):
            hears = jnp.logical_and(hears, peer // 2 != 1)

        @pl.when(hears)
        def _():
            pl.semaphore_signal(ready_tm.at[d - 1], inc=1, device_id=(peer, my_region), device_id_type=MESH)
    for r, peer in obs_peers:
        @pl.when(peer < my_region)
        def _():
            pl.semaphore_signal(ready_obs, inc=1, device_id=(me, peer), device_id_type=MESH)
    small[0].wait()
    small[1].wait()

    def request(d):
        return pltpu.make_async_remote_copy(
            src_ref=own, dst_ref=idx.at[d],
            send_sem=idx_send, recv_sem=idx_recv.at[d - 1],
            device_id=(flip(me, d), my_region), device_id_type=MESH,
        )

    def ask(d):
        @pl.when(jnp.logical_and(flip(me, d) > me, jnp.logical_not(opposite(d))))
        def _():
            pl.semaphore_wait(ready_tm.at[d - 1], 1)

        request(d).start()

    def pass_on(e):
        return pltpu.make_async_remote_copy(
            src_ref=idx.at[ACROSS], dst_ref=idx.at[e ^ ACROSS],
            send_sem=pass_send, recv_sem=idx_recv.at[(e ^ ACROSS) - 1],
            device_id=(flip(me, e), my_region), device_id_type=MESH,
        )

    def move(d, k, count=1, first=0):
        part, rows = pl.ds(d * GCAP + k, count), pl.ds(first, columns - first)
        return pltpu.make_async_remote_copy(
            src_ref=send.at[part, rows], dst_ref=recv.at[part, rows],
            send_sem=dat_send, recv_sem=dat_recv.at[d - 1 if d != ACROSS or k == 0 else windows - 2 + k],
            device_id=(flip(me, d), my_region), device_id_type=MESH,
        )

    def moved(count):
        part = send.at[pl.ds(0, count)]
        pltpu.make_async_remote_copy(
            src_ref=part, dst_ref=part, send_sem=dat_send, recv_sem=dat_recv.at[0],
            device_id=(flip(me, 1), my_region), device_id_type=MESH,
        ).wait_send()

    def give(d, first=0, skip_heard=None):
        if d != skip_heard:
            request(d).wait_recv()
        named = last_hits(lambda g: idx[d, 0, g], lambda g: idx[d, 1, g], groups, me, 0)
        for k in range(GCAP):
            send[d * GCAP + k, first:] = slab[named[k], first:]
            if d == ACROSS:
                move(d, k, 1, first).start()
        if d != ACROSS:
            move(d, 0, GCAP, first).start()

    def run_ahead():
        return pltpu.make_async_remote_copy(
            src_ref=head, dst_ref=pre, send_sem=pre_send, recv_sem=pre_recv,
            device_id=(flip(me, ACROSS), my_region), device_id_type=MESH,
        )

    def hand_on(e):
        return pltpu.make_async_remote_copy(
            src_ref=on_out.at[e], dst_ref=on_in.at[e ^ ACROSS],
            send_sem=on_send, recv_sem=on_recv.at[e % 2],
            device_id=(flip(me, e), my_region), device_id_type=MESH,
        )

    def relay():
        run_ahead().wait_recv()
        for e in (1, 2, 3):
            named = last_hits(
                lambda g: idx[e, 0, g], lambda g: idx[e, 1, g], groups, flip(me, ACROSS), 0
            )
            for k in range(GCAP):
                on_out[e, k] = pre[named[k]]
            hand_on(e).start()

    if tuned:
        for z, order in enumerate(ASK):
            @pl.when(me // 2 == z)
            def _():
                for d in order:
                    ask(d)
                    if d == AHEAD_AFTER[z]:
                        head_in.wait()
                        run_ahead().start()
                if z in (0, 3):
                    head_in.wait()
                if z == 2:
                    request(ACROSS).wait_recv()
                    for e in (1, 2, 3):
                        pass_on(e).start()
    else:
        for d in range(1, windows):
            ask(d)
    later = regions - 2 - 2 * (my_region // 2)

    @pl.when(later > 0)
    def _():
        pl.semaphore_wait(ready_obs, later)

    slab_in.wait()
    wts_in.start()
    obs_in.start()
    if tuned:
        @pl.when(inner)
        def _():
            for d in INNER_GIVE:
                give(d)

        @pl.when(jnp.logical_not(inner))
        def _():
            for d in OUTER_GIVE:
                give(d)
    else:
        for d in range(1, windows):
            give(d)

    for copy in small[2:]:
        copy.wait()

    def fill(w, carry):
        named = last_hits(lambda g: own[0, g], lambda g: g, groups, w, -1)
        for k in range(GCAP):
            table[w * GCAP + k] = named[k]
        return carry

    lax.fori_loop(0, windows, fill, 0)

    def place(g, carry):
        base = own[0, g] * GCAP
        rank = jnp.int32(0)
        for k in range(1, GCAP):
            rank = rank + jnp.where(table[base + k] == g, k, 0)
        slot_tab[g] = base + rank
        return carry

    lax.fori_loop(0, groups, place, 0)

    down = lax.broadcasted_iota(jnp.int32, (slots, slots), 0)
    across = lax.broadcasted_iota(jnp.int32, (slots, slots), 1)
    lane = lax.broadcasted_iota(jnp.int32, (1, slots), 1)
    ones = jnp.ones((slots, levels), jnp.bfloat16)

    def spread(g, carry):
        row = jnp.where(lane < counts[g], flags[pl.ds(g, 1), :], 0)
        diagonal = jnp.where(down == across, jnp.broadcast_to(row, (slots, slots)), 0)
        mask[g] = jnp.dot(
            diagonal.astype(jnp.float32).astype(jnp.bfloat16), ones,
            preferred_element_type=jnp.float32,
        )
        return carry

    lax.fori_loop(0, groups, spread, 0)
    wts_in.wait()
    obs_in.wait()
    inverse = inv[...]
    padded = windows * GCAP > groups

    def check(w, blocks):
        one = jnp.zeros((1, levels), jnp.float32)
        two = jnp.zeros((1, levels), jnp.float32)
        kept = jnp.zeros((1, levels), jnp.float32)
        for k in range(GCAP):
            named = table[w * GCAP + k]
            g = jnp.maximum(named, 0)
            hx = jnp.dot(wts[g], blocks(k, g), preferred_element_type=jnp.float32)
            keep = mask[g]
            if padded:
                keep = keep * jnp.where(named >= 0, 1.0, 0.0)
            dep = keep * (obs[g].astype(jnp.float32) - hx) * inverse
            dep_slot[w * GCAP + k] = dep.astype(jnp.bfloat16)
            one = one + jnp.sum(dep, 0, keepdims=True)
            two = two + jnp.sum(dep * dep, 0, keepdims=True)
            kept = kept + jnp.sum(keep, 0, keepdims=True)
        stat_send[w] = jnp.concatenate([one, two, kept] + [kept] * (stat_send.shape[1] - 3), 0)

    def share(w, first):
        for r in reversed(range(first, regions)):
            copy = pltpu.make_async_remote_copy(
                src_ref=stat_send.at[w], dst_ref=stat_recv.at[flat],
                send_sem=st_send, recv_sem=st_recv,
                device_id=(w, flip(my_region, r)), device_id_type=MESH,
            )
            copy.start()

    check(me, lambda k, g: slab[own[1, g]])
    share(me, 1)

    def take(d, first=0):
        w = flip(me, d)
        if first and d != ACROSS:
            hand_on(d ^ ACROSS).wait_recv()

        if d != ACROSS:
            move(d, 0, GCAP, first).wait_recv()

        def arrived(k, g):
            if first:
                recv[d * GCAP + k, :first] = pre[own[1, g]] if d == ACROSS else on_in[d, k]
            if d == ACROSS:
                move(d, k, 1, first).wait_recv()
            return recv[d * GCAP + k]

        check(w, arrived)
        share(w, 0)

    if tuned:
        @pl.when(inner)
        def _():
            for d in INNER_TAKE[0]:
                take(d)
            for d in INNER_LATE:
                if d == ACROSS:
                    @pl.when(me // 2 == 1)
                    def _():
                        request(ACROSS).wait_recv()
                give(d, ahead, ACROSS)

            relay()
            for d in INNER_TAKE[1]:
                take(d, ahead if d in (6, 7) else 0)
            moved(len(INNER_GIVE) * GCAP + len(INNER_LATE) * GCAP * (columns - ahead) // columns)
            run_ahead().wait_send()
            part = on_out.at[pl.ds(1, 3)]
            pltpu.make_async_remote_copy(
                src_ref=part, dst_ref=part, send_sem=on_send, recv_sem=on_recv.at[0],
                device_id=(flip(me, 1), my_region), device_id_type=MESH,
            ).wait_send()

        @pl.when(jnp.logical_not(inner))
        def _():
            for d in OUTER_TAKE:
                take(d, ahead if d in (4, 5) else 0)
            moved(len(OUTER_GIVE) * GCAP)
    else:
        for d in range(1, windows):
            take(d)
        moved((windows - 1) * GCAP)

    def permute(g, carry):
        dep_out[g] = dep_slot[slot_tab[g]]
        return carry

    lax.fori_loop(0, groups, permute, 0, unroll=4)

    def asked(count, sem):
        part = idx.at[pl.ds(0, count)]
        pltpu.make_async_remote_copy(
            src_ref=part, dst_ref=part, send_sem=sem, recv_sem=idx_recv.at[0],
            device_id=(flip(me, 1), my_region), device_id_type=MESH,
        ).wait_send()

    if tuned:
        for z, order in enumerate(ASK):
            @pl.when(me // 2 == z)
            def _():
                asked(len(order), idx_send)
                if z == 2:
                    asked(3, pass_send)
    else:
        asked(windows - 1, idx_send)

    rest = pl.ds(0, everyone - 1)
    everything = pltpu.make_async_remote_copy(
        src_ref=stat_recv.at[rest], dst_ref=stat_recv.at[rest],
        send_sem=st_send, recv_sem=st_recv,
        device_id=(flip(me, 1), my_region), device_id_type=MESH,
    )
    everything.wait_recv()
    stat_recv[flat] = stat_send[me]
    total_out[...] = jnp.sum(stat_recv[...], 0)
    everything.wait_send()


def finish(dep, total, dep_out, bias_out, chi_out, ratio, sems):
    whole = pltpu.make_async_copy(dep, dep_out, sems.at[0])
    whole.start()
    weight = total[2:3] + 1.0
    ratio[0:1] = total[0:1] / jnp.sqrt(weight)
    ratio[8:9] = total[1:2] / weight
    bias = pltpu.make_async_copy(ratio.at[0:1], bias_out, sems.at[1])
    chi = pltpu.make_async_copy(ratio.at[8:9], chi_out, sems.at[2])
    bias.start()
    chi.start()
    bias.wait()
    chi.wait()
    whole.wait()


def per_device(trajectory, weights, observed, window, block, counts, flags, inv_error):
    windows = lax.axis_size("tm")
    regions = lax.axis_size("obs")
    groups, slots, columns = weights.shape
    levels = observed.shape[2]
    blocks = trajectory.shape[1]
    dma = pltpu.SemaphoreType.DMA
    regular = pltpu.SemaphoreType.REGULAR
    hbm = pl.BlockSpec(memory_space=pl.ANY)
    vmem = pl.BlockSpec(memory_space=pltpu.VMEM)
    b16, f32, i32 = jnp.bfloat16, jnp.float32, jnp.int32
    departures, total = pl.pallas_call(
        functools.partial(kernel, windows, regions, groups, slots, levels),
        out_shape=(
            pltpu.VMEM((groups, slots, levels), b16),
            pltpu.VMEM((3, levels), f32),
        ),
        in_specs=[hbm] * 8,
        out_specs=(vmem, vmem),
        scratch_shapes=[
            pltpu.VMEM((blocks, columns, levels), b16),
            pltpu.VMEM((groups, slots, columns), b16),
            pltpu.VMEM((groups, slots, levels), b16),
            pltpu.VMEM((windows * GCAP, columns, levels), b16),
            pltpu.VMEM((windows * GCAP, columns, levels), b16),
            pltpu.VMEM((blocks, columns // AHEAD, levels), b16),
            pltpu.VMEM((blocks, columns // AHEAD, levels), b16),
            pltpu.VMEM((windows, GCAP, columns // AHEAD, levels), b16),
            pltpu.VMEM((windows, GCAP, columns // AHEAD, levels), b16),
            pltpu.VMEM((groups, slots, levels), f32),
            pltpu.VMEM((windows * GCAP, slots, levels), b16),
            pltpu.VMEM((windows, 3, levels), f32),
            pltpu.VMEM((windows * regions, 3, levels), f32),
            pltpu.SMEM((windows, 2, groups), i32),
            pltpu.SMEM((2, groups), i32),
            pltpu.SMEM((windows * GCAP,), i32),
            pltpu.SMEM((groups,), i32),
            pltpu.SMEM((groups,), i32),
            pltpu.VMEM((groups, slots), i32),
            pltpu.VMEM((1, levels), f32),
            dma((9,)),
            regular((windows - 1,)),
            regular,
            dma,
            dma((windows - 1,)),
            dma,
            dma,
            dma((windows + GCAP - 2,)),
            dma,
            dma,
            dma,
            dma((2,)),
            dma,
            dma,
        ],
        compiler_params=pltpu.CompilerParams(
            collective_id=0, has_side_effects=True, vmem_limit_bytes=60 * 1024 * 1024
        ),
    )(
        trajectory, weights, observed, window[:, 0], block, counts, flags,
        inv_error.reshape(1, levels),
    )
    return pl.pallas_call(
        finish,
        out_shape=(
            jax.ShapeDtypeStruct((groups, slots, levels), b16),
            jax.ShapeDtypeStruct((1, levels), f32),
            jax.ShapeDtypeStruct((1, levels), f32),
        ),
        in_specs=[vmem, vmem],
        out_specs=(hbm, hbm, hbm),
        scratch_shapes=[pltpu.VMEM((16, levels), f32), dma((3,))],
    )(*(pltpu.with_memory_space_constraint(x, pltpu.VMEM) for x in (departures, total)))


def solution(mesh):
    return jax.shard_map(
        per_device,
        mesh=mesh,
        in_specs=(
            P("tm", "obs", None, None),
            P(("tm", "obs"), None, None),
            P(("tm", "obs"), None, None),
            P(("tm", "obs"), None),
            P(("tm", "obs")),
            P(("tm", "obs")),
            P(("tm", "obs"), None),
            P(),
        ),
        out_specs=(P(("tm", "obs"), None, None), P("tm", None), P("tm", None)),
        check_vma=False,
    )
```

```python
import functools

import jax
import jax.numpy as jnp
from jax import lax
from jax.experimental import pallas as pl
from jax.experimental.pallas import tpu as pltpu
from jax.sharding import PartitionSpec as P

GCAP = 4
MESH = pl.DeviceIdType.MESH

ASK = ((1, 2, 3, 4, 5, 6, 7), (6, 2, 3, 1), (4, 5, 7, 6, 1, 2, 3), (2, 3, 4, 5, 6, 7, 1))
AHEAD_AFTER = (None, 6, 6, None)
OUTER_GIVE, OUTER_TAKE = (5, 4, 1, 7, 6, 3, 2), (1, 2, 3, 7, 6, 4, 5)
INNER_GIVE, INNER_LATE, INNER_TAKE = (1, 2, 3), (4, 5, 7, 6), ((1, 5, 4), (3, 2, 7, 6))
ACROSS, AHEAD = 6, 4


def flip(index, pattern):
    bit, moved = 1, index
    while bit <= 64:
        moved = moved + bit * ((pattern // bit) % 2) * (1 - 2 * ((index // bit) % 2))
        bit *= 2
    return moved


def last_hits(win_of, value_of, groups, wanted, start):
    def step(g, held):
        hit = win_of(g) == wanted
        shifted = (value_of(g),) + held[:-1]
        return tuple(jnp.where(hit, new, old) for new, old in zip(shifted, held))

    return lax.fori_loop(0, groups, step, (jnp.int32(start),) * GCAP, unroll=8)


def kernel(
    windows, regions, groups, slots, levels,
    traj, weights, observed, win_in, blk_in, counts_in, flags_in, inv_in,
    dep_out, total_out,
    slab, wts, obs, send, recv, head, pre, on_out, on_in, mask, dep_slot, stat_send, stat_recv,
    idx, own, table, slot_tab, counts, flags, inv,
    in_sems, ready_tm, ready_obs, idx_send, idx_recv, pass_send, dat_send, dat_recv,
    pre_send, pre_recv, on_send, on_recv, st_send, st_recv,
):
    me = lax.axis_index("tm")
    my_region = lax.axis_index("obs")
    everyone = windows * regions
    flat = me * regions + my_region
    tuned = windows == 8
    inner_flag = ((me // 2 + 1) // 2) % 2
    inner = inner_flag == 1
    blocks, columns = slab.shape[0], slab.shape[1]
    ahead = columns // AHEAD if tuned else 0

    small = [
        pltpu.make_async_copy(src, dst, in_sems.at[3 + n])
        for n, (src, dst) in enumerate(
            ((win_in, own.at[0]), (blk_in, own.at[1]), (counts_in, counts), (flags_in, flags), (inv_in, inv))
        )
    ]
    slab_in = pltpu.make_async_copy(traj.at[0], slab, in_sems.at[0])
    head_in = pltpu.make_async_copy(traj.at[0, :, pl.ds(0, columns // AHEAD)], head, in_sems.at[8])
    wts_in = pltpu.make_async_copy(weights, wts, in_sems.at[1])
    obs_in = pltpu.make_async_copy(observed, obs, in_sems.at[2])

    barrier = pltpu.get_barrier_semaphore()

    def opposite(d):
        return jnp.logical_and(inner, tuned and d == ACROSS)

    tm_peers = [(d, flip(me, d)) for d in range(1, windows)]
    obs_peers = [(r, flip(my_region, r)) for r in range(2, regions)]
    pl.semaphore_signal(barrier, inc=1, device_id=(me, flip(my_region, 1)), device_id_type=MESH)
    for d, peer in tm_peers:
        @pl.when(jnp.logical_or(peer > me, opposite(d)))
        def _():
            pl.semaphore_signal(barrier, inc=1, device_id=(peer, my_region), device_id_type=MESH)
    for r, peer in obs_peers:
        @pl.when(peer > my_region)
        def _():
            pl.semaphore_signal(barrier, inc=1, device_id=(me, peer), device_id_type=MESH)
    small[0].start()
    small[1].start()
    if tuned:
        head_in.start()
    slab_in.start()
    for copy in small[2:]:
        copy.start()
    early = 1 + me + 2 * (my_region // 2)
    if tuned:
        early = early + inner_flag * (2 - me // 2)
    pl.semaphore_wait(barrier, early)
    for d, peer in tm_peers:
        hears = jnp.logical_and(peer < me, jnp.logical_not(opposite(d)))
        if tuned and d in (4, 5, 7):
            hears = jnp.logical_and(hears, peer // 2 != 1)

        @pl.when(hears)
        def _():
            pl.semaphore_signal(ready_tm.at[d - 1], inc=1, device_id=(peer, my_region), device_id_type=MESH)
    for r, peer in obs_peers:
        @pl.when(peer < my_region)
        def _():
            pl.semaphore_signal(ready_obs, inc=1, device_id=(me, peer), device_id_type=MESH)
    small[0].wait()
    small[1].wait()

    def request(d):
        return pltpu.make_async_remote_copy(
            src_ref=own, dst_ref=idx.at[d],
            send_sem=idx_send, recv_sem=idx_recv.at[d - 1],
            device_id=(flip(me, d), my_region), device_id_type=MESH,
        )

    def ask(d):
        @pl.when(jnp.logical_and(flip(me, d) > me, jnp.logical_not(opposite(d))))
        def _():
            pl.semaphore_wait(ready_tm.at[d - 1], 1)

        request(d).start()

    def pass_on(e):
        return pltpu.make_async_remote_copy(
            src_ref=idx.at[ACROSS], dst_ref=idx.at[e ^ ACROSS],
            send_sem=pass_send, recv_sem=idx_recv.at[(e ^ ACROSS) - 1],
            device_id=(flip(me, e), my_region), device_id_type=MESH,
        )

    def move(d, k, count=1, first=0):
        part, rows = pl.ds(d * GCAP + k, count), pl.ds(first, columns - first)
        return pltpu.make_async_remote_copy(
            src_ref=send.at[part, rows], dst_ref=recv.at[part, rows],
            send_sem=dat_send, recv_sem=dat_recv.at[d - 1 if d != ACROSS or k == 0 else windows - 2 + k],
            device_id=(flip(me, d), my_region), device_id_type=MESH,
        )

    def moved(count):
        part = send.at[pl.ds(0, count)]
        pltpu.make_async_remote_copy(
            src_ref=part, dst_ref=part, send_sem=dat_send, recv_sem=dat_recv.at[0],
            device_id=(flip(me, 1), my_region), device_id_type=MESH,
        ).wait_send()

    def give(d, first=0, skip_heard=None):
        if d != skip_heard:
            request(d).wait_recv()
        named = last_hits(lambda g: idx[d, 0, g], lambda g: idx[d, 1, g], groups, me, 0)
        for k in range(GCAP):
            send[d * GCAP + k, first:] = slab[named[k], first:]
            if d == ACROSS:
                move(d, k, 1, first).start()
        if d != ACROSS:
            move(d, 0, GCAP, first).start()

    def run_ahead():
        return pltpu.make_async_remote_copy(
            src_ref=head, dst_ref=pre, send_sem=pre_send, recv_sem=pre_recv,
            device_id=(flip(me, ACROSS), my_region), device_id_type=MESH,
        )

    def hand_on(e):
        return pltpu.make_async_remote_copy(
            src_ref=on_out.at[e], dst_ref=on_in.at[e ^ ACROSS],
            send_sem=on_send, recv_sem=on_recv.at[e % 2],
            device_id=(flip(me, e), my_region), device_id_type=MESH,
        )

    def relay():
        run_ahead().wait_recv()
        for e in (1, 2, 3):
            named = last_hits(
                lambda g: idx[e, 0, g], lambda g: idx[e, 1, g], groups, flip(me, ACROSS), 0
            )
            for k in range(GCAP):
                on_out[e, k] = pre[named[k]]
            hand_on(e).start()

    if tuned:
        for z, order in enumerate(ASK):
            @pl.when(me // 2 == z)
            def _():
                for d in order:
                    ask(d)
                    if d == AHEAD_AFTER[z]:
                        head_in.wait()
                        run_ahead().start()
                if z in (0, 3):
                    head_in.wait()
                if z == 2:
                    request(ACROSS).wait_recv()
                    for e in (1, 2, 3):
                        pass_on(e).start()
    else:
        for d in range(1, windows):
            ask(d)
    later = regions - 2 - 2 * (my_region // 2)

    @pl.when(later > 0)
    def _():
        pl.semaphore_wait(ready_obs, later)

    slab_in.wait()
    wts_in.start()
    obs_in.start()
    if tuned:
        @pl.when(inner)
        def _():
            for d in INNER_GIVE:
                give(d)

        @pl.when(jnp.logical_not(inner))
        def _():
            for d in OUTER_GIVE:
                give(d)
    else:
        for d in range(1, windows):
            give(d)

    for copy in small[2:]:
        copy.wait()

    def fill(w, carry):
        named = last_hits(lambda g: own[0, g], lambda g: g, groups, w, -1)
        for k in range(GCAP):
            table[w * GCAP + k] = named[k]
        return carry

    lax.fori_loop(0, windows, fill, 0)

    def place(g, carry):
        base = own[0, g] * GCAP
        rank = jnp.int32(0)
        for k in range(1, GCAP):
            rank = rank + jnp.where(table[base + k] == g, k, 0)
        slot_tab[g] = base + rank
        return carry

    lax.fori_loop(0, groups, place, 0)

    down = lax.broadcasted_iota(jnp.int32, (slots, slots), 0)
    across = lax.broadcasted_iota(jnp.int32, (slots, slots), 1)
    lane = lax.broadcasted_iota(jnp.int32, (1, slots), 1)
    ones = jnp.ones((slots, levels), jnp.bfloat16)

    def spread(g, carry):
        row = jnp.where(lane < counts[g], flags[pl.ds(g, 1), :], 0)
        diagonal = jnp.where(down == across, jnp.broadcast_to(row, (slots, slots)), 0)
        mask[g] = jnp.dot(
            diagonal.astype(jnp.float32).astype(jnp.bfloat16), ones,
            preferred_element_type=jnp.float32,
        )
        return carry

    lax.fori_loop(0, groups, spread, 0)
    wts_in.wait()
    obs_in.wait()
    inverse = inv[...]
    padded = windows * GCAP > groups

    def check(w, blocks):
        one = jnp.zeros((1, levels), jnp.float32)
        two = jnp.zeros((1, levels), jnp.float32)
        kept = jnp.zeros((1, levels), jnp.float32)
        for k in range(GCAP):
            named = table[w * GCAP + k]
            g = jnp.maximum(named, 0)
            hx = jnp.dot(wts[g], blocks(k, g), preferred_element_type=jnp.float32)
            keep = mask[g]
            if padded:
                keep = keep * jnp.where(named >= 0, 1.0, 0.0)
            dep = keep * (obs[g].astype(jnp.float32) - hx) * inverse
            dep_slot[w * GCAP + k] = dep.astype(jnp.bfloat16)
            one = one + jnp.sum(dep, 0, keepdims=True)
            two = two + jnp.sum(dep * dep, 0, keepdims=True)
            kept = kept + jnp.sum(keep, 0, keepdims=True)
        stat_send[w] = jnp.concatenate([one, two, kept] + [kept] * (stat_send.shape[1] - 3), 0)

    def share(w, first):
        for r in reversed(range(first, regions)):
            copy = pltpu.make_async_remote_copy(
                src_ref=stat_send.at[w], dst_ref=stat_recv.at[flat],
                send_sem=st_send, recv_sem=st_recv,
                device_id=(w, flip(my_region, r)), device_id_type=MESH,
            )
            copy.start()

    check(me, lambda k, g: slab[own[1, g]])
    share(me, 1)

    def take(d, first=0):
        w = flip(me, d)
        if first and d != ACROSS:
            hand_on(d ^ ACROSS).wait_recv()

        if d != ACROSS:
            move(d, 0, GCAP, first).wait_recv()

        def arrived(k, g):
            if first:
                recv[d * GCAP + k, :first] = pre[own[1, g]] if d == ACROSS else on_in[d, k]
            if d == ACROSS:
                move(d, k, 1, first).wait_recv()
            return recv[d * GCAP + k]

        check(w, arrived)
        share(w, 0)

    if tuned:
        @pl.when(inner)
        def _():
            for d in INNER_TAKE[0]:
                take(d)
            for d in INNER_LATE:
                if d == ACROSS:
                    @pl.when(me // 2 == 1)
                    def _():
                        request(ACROSS).wait_recv()
                give(d, ahead, ACROSS)

            relay()
            for d in INNER_TAKE[1]:
                take(d, ahead if d in (6, 7) else 0)
            moved(len(INNER_GIVE) * GCAP + len(INNER_LATE) * GCAP * (columns - ahead) // columns)
            run_ahead().wait_send()
            part = on_out.at[pl.ds(1, 3)]
            pltpu.make_async_remote_copy(
                src_ref=part, dst_ref=part, send_sem=on_send, recv_sem=on_recv.at[0],
                device_id=(flip(me, 1), my_region), device_id_type=MESH,
            ).wait_send()

        @pl.when(jnp.logical_not(inner))
        def _():
            for d in OUTER_TAKE:
                take(d, ahead if d in (4, 5) else 0)
            moved(len(OUTER_GIVE) * GCAP)
    else:
        for d in range(1, windows):
            take(d)
        moved((windows - 1) * GCAP)

    def permute(g, carry):
        dep_out[g] = dep_slot[slot_tab[g]]
        return carry

    lax.fori_loop(0, groups, permute, 0, unroll=4)

    def asked(count, sem):
        part = idx.at[pl.ds(0, count)]
        pltpu.make_async_remote_copy(
            src_ref=part, dst_ref=part, send_sem=sem, recv_sem=idx_recv.at[0],
            device_id=(flip(me, 1), my_region), device_id_type=MESH,
        ).wait_send()

    if tuned:
        for z, order in enumerate(ASK):
            @pl.when(me // 2 == z)
            def _():
                asked(len(order), idx_send)
                if z == 2:
                    asked(3, pass_send)
    else:
        asked(windows - 1, idx_send)

    rest = pl.ds(0, everyone - 1)
    everything = pltpu.make_async_remote_copy(
        src_ref=stat_recv.at[rest], dst_ref=stat_recv.at[rest],
        send_sem=st_send, recv_sem=st_recv,
        device_id=(flip(me, 1), my_region), device_id_type=MESH,
    )
    everything.wait_recv()
    stat_recv[flat] = stat_send[me]
    total_out[...] = jnp.sum(stat_recv[...], 0)
    everything.wait_send()


def finish(dep, total, dep_out, bias_out, chi_out, ratio, sems):
    whole = pltpu.make_async_copy(dep, dep_out, sems.at[0])
    whole.start()
    weight = total[2:3] + 1.0
    ratio[0:1] = total[0:1] / jnp.sqrt(weight)
    ratio[8:9] = total[1:2] / weight
    bias = pltpu.make_async_copy(ratio.at[0:1], bias_out, sems.at[1])
    chi = pltpu.make_async_copy(ratio.at[8:9], chi_out, sems.at[2])
    bias.start()
    chi.start()
    bias.wait()
    chi.wait()
    whole.wait()


def per_device(trajectory, weights, observed, window, block, counts, flags, inv_error):
    windows = lax.axis_size("tm")
    regions = lax.axis_size("obs")
    groups, slots, columns = weights.shape
    levels = observed.shape[2]
    blocks = trajectory.shape[1]
    dma = pltpu.SemaphoreType.DMA
    regular = pltpu.SemaphoreType.REGULAR
    hbm = pl.BlockSpec(memory_space=pl.ANY)
    vmem = pl.BlockSpec(memory_space=pltpu.VMEM)
    b16, f32, i32 = jnp.bfloat16, jnp.float32, jnp.int32
    departures, total = pl.pallas_call(
        functools.partial(kernel, windows, regions, groups, slots, levels),
        out_shape=(
            pltpu.VMEM((groups, slots, levels), b16),
            pltpu.VMEM((3, levels), f32),
        ),
        in_specs=[hbm] * 8,
        out_specs=(vmem, vmem),
        scratch_shapes=[
            pltpu.VMEM((blocks, columns, levels), b16),
            pltpu.VMEM((groups, slots, columns), b16),
            pltpu.VMEM((groups, slots, levels), b16),
            pltpu.VMEM((windows * GCAP, columns, levels), b16),
            pltpu.VMEM((windows * GCAP, columns, levels), b16),
            pltpu.VMEM((blocks, columns // AHEAD, levels), b16),
            pltpu.VMEM((blocks, columns // AHEAD, levels), b16),
            pltpu.VMEM((windows, GCAP, columns // AHEAD, levels), b16),
            pltpu.VMEM((windows, GCAP, columns // AHEAD, levels), b16),
            pltpu.VMEM((groups, slots, levels), f32),
            pltpu.VMEM((windows * GCAP, slots, levels), b16),
            pltpu.VMEM((windows, 3, levels), f32),
            pltpu.VMEM((windows * regions, 3, levels), f32),
            pltpu.SMEM((windows, 2, groups), i32),
            pltpu.SMEM((2, groups), i32),
            pltpu.SMEM((windows * GCAP,), i32),
            pltpu.SMEM((groups,), i32),
            pltpu.SMEM((groups,), i32),
            pltpu.VMEM((groups, slots), i32),
            pltpu.VMEM((1, levels), f32),
            dma((9,)),
            regular((windows - 1,)),
            regular,
            dma,
            dma((windows - 1,)),
            dma,
            dma,
            dma((windows + GCAP - 2,)),
            dma,
            dma,
            dma,
            dma((2,)),
            dma,
            dma,
        ],
        compiler_params=pltpu.CompilerParams(
            collective_id=0, has_side_effects=True, vmem_limit_bytes=60 * 1024 * 1024
        ),
    )(
        trajectory, weights, observed, window[:, 0], block, counts, flags,
        inv_error.reshape(1, levels),
    )
    return pl.pallas_call(
        finish,
        out_shape=(
            jax.ShapeDtypeStruct((groups, slots, levels), b16),
            jax.ShapeDtypeStruct((1, levels), f32),
            jax.ShapeDtypeStruct((1, levels), f32),
        ),
        in_specs=[vmem, vmem],
        out_specs=(hbm, hbm, hbm),
        scratch_shapes=[pltpu.VMEM((16, levels), f32), dma((3,))],
    )(*(pltpu.with_memory_space_constraint(x, pltpu.VMEM) for x in (departures, total)))


def solution(mesh):
    return jax.shard_map(
        per_device,
        mesh=mesh,
        in_specs=(
            P("tm", "obs", None, None),
            P(("tm", "obs"), None, None),
            P(("tm", "obs"), None, None),
            P(("tm", "obs"), None),
            P(("tm", "obs")),
            P(("tm", "obs")),
            P(("tm", "obs"), None),
            P(),
        ),
        out_specs=(P(("tm", "obs"), None, None), P("tm", None), P("tm", None)),
        check_vma=False,
    )
```
